32 devices in a mesh: row: 4 (over z), col: 4 (over y, x), layer: 2 (over core).
Axes of the slice: x: 2, y: 2, z: 4, core: 2. Of those that a mesh axis runs over, the one named last changes fastest.
Arguments:
- matrix: float32 [16, 512, 16, 512], P('row', None, 'col', 'layer'), may hold values from -40 to 40, as said below
- transforms: float32 [1, 8, 1024, 1024], P(None, 'row', ('col', 'layer')), may hold values from -0.1875 to 0.1875
Outputs:
- swept: float32 [16, 512, 16, 512], P('row', None, 'col', 'layer')
The draws below stay inside these ranges and needn't reach their ends.
Inputs may be any that keep to these rules, and one draw needn't show every extreme that they name: `matrix`: symmetric: entry [i, a, j, b] equals entry [j, b, i, a].
All inputs are finite; a program needn't handle non-finite values.
Results may differ from the reference program's by a relative error of at most 0.0001.
Values sent between devices are 32-bit elements; how exact they have to be, the bound alone decides.
A program may use at most 192 MiB of HBM per device.

```python
import jax
import jax.numpy as jnp
from jax import lax

BS = 512
STEPS = 1
PAIRS = 8
NBLK = 16


def draw_matrix(key, part):
    gaussian = jax.random.normal(key, (NBLK * BS, NBLK * BS), jnp.float32)
    symmetric = (gaussian + gaussian.T) * 0.7071067811865476
    return symmetric.reshape(NBLK, BS, NBLK, BS)


def steps_of(own_key, dims, pieces, low, largest):
    def one(position, parts):
        heights = jax.random.uniform(jax.random.fold_in(jax.random.fold_in(own_key, 6), position), (parts,), jnp.float32, low / len(pieces), largest / len(pieces))
        return jnp.repeat(jnp.exp(heights), dims[position] // parts).reshape((-1,) + (1,) * (len(dims) - position - 1))

    factor_of = one(*pieces[0])
    for cut in pieces[1:]:
        factor_of = factor_of * one(*cut)
    return factor_of


def centred(own_key, dims, spread, limit, pieces=(), held_as=jnp.bfloat16):
    loudness = steps_of(own_key, dims, pieces, -0.22, 0.18) if pieces else 1.0
    result = jax.random.normal(own_key, dims, jnp.float32) * spread * loudness
    return jnp.minimum(jnp.maximum(result, -limit), limit).astype(held_as)


def setup_inputs(seed: int = 0) -> dict:
    keys = jax.random.split(jax.random.key(seed), 3)
    matrix = draw_matrix(jax.random.fold_in(keys[2], 71), 0)
    transforms = centred(keys[1], (STEPS, PAIRS, 2 * BS, 2 * BS), (2 * BS) ** -0.5, 0.1875, ((1, 4), (2, 8)), jnp.float32)
    return dict(matrix=matrix, transforms=transforms)


def sweep_order(count):
    slot_ids = jnp.arange(count, dtype=jnp.int32)
    is_odd = slot_ids % 2
    source = jnp.where(is_odd == 0, slot_ids - 2, slot_ids + 2)
    source = jnp.where(slot_ids == 0, 0, source)
    source = jnp.where(slot_ids == 2, 1, source)
    source = jnp.where(slot_ids == count - 1, count - 2, source)
    return source.astype(jnp.int32)


def reference(matrix, transforms):
    source = sweep_order(NBLK)
    current = matrix
    for step_index in range(STEPS):
        blocks = transforms[step_index]
        grouped = current.reshape(PAIRS, 2 * BS, PAIRS, 2 * BS)
        left_part = jnp.einsum("pkqb,pka->paqb", grouped, blocks, precision=lax.Precision.HIGHEST)
        rotated_pairs = jnp.einsum("paqk,qkb->paqb", left_part, blocks, precision=lax.Precision.HIGHEST)
        rotated = rotated_pairs.reshape(NBLK, BS, NBLK, BS)
        current = jnp.take(jnp.take(rotated, source, axis=0), source, axis=2)
    return current
```

```python
import jax
import jax.numpy as jnp
from jax import lax
from jax.sharding import PartitionSpec as P


three_pass = lax.Precision.HIGH


def shifted(block, axis, distance):
    devices = range(lax.axis_size(axis))
    route = [(i - distance, i) for i in devices if i - distance in devices]
    return lax.ppermute(block, axis, route)


def crossed(block, axis, mask):
    return lax.ppermute(block, axis, [(i, i ^ mask) for i in range(lax.axis_size(axis))])


def rearranged(slots, from_prev, from_next, position, count):
    width = len(slots)
    result = [jnp.where(position == 0, slots[0], from_prev)]
    for local in range(1, width):
        if local % 2 == 1:
            if local == width - 1:
                result.append(jnp.where(position == count - 1, slots[width - 2], from_next))
            else:
                result.append(slots[local + 2])
        else:
            result.append(jnp.where(position == 0, slots[1], slots[0]))
    return result


def by_layer(mine, other, layer_pos, axis):
    low = jnp.where(layer_pos == 0, mine, other)
    high = jnp.where(layer_pos == 0, other, mine)
    return jnp.stack([low, high], axis)


def product(a, b):
    return lax.dot_general(
        a, b, (((1,), (0,)), ((), ())), precision=three_pass, preferred_element_type=jnp.float32
    )


def shards(matrix, transforms):
    width, block_size, _, half_width = matrix.shape
    pair_dev = width // 2
    rows_n = lax.axis_size("row")
    cols_n = lax.axis_size("col")
    row_pos = lax.axis_index("row")
    col_pos = lax.axis_index("col")
    layer_pos = lax.axis_index("layer")
    own = transforms[0]
    piece = own.shape[1]
    order = 2 * block_size

    ups, downs = [own], [own]
    for _ in range(rows_n - 1):
        ups.append(shifted(ups[-1], "row", 1))
        downs.append(shifted(downs[-1], "row", -1))

    gathered = jnp.zeros((pair_dev, cols_n, piece, order), jnp.float32)
    for mask in range(cols_n):
        part = own if mask == 0 else crossed(own, "col", mask)
        gathered = lax.dynamic_update_slice(gathered, part[:, None], (0, col_pos ^ mask, 0, 0))
    panel = by_layer(gathered, crossed(gathered, "layer", 1), layer_pos, 2)
    panel = panel.reshape(pair_dev, order, order)

    grouped = matrix.reshape(pair_dev, order, width, half_width)
    left = []
    for p in range(pair_dev):
        flat = grouped[p].reshape(order, width * half_width)
        left.append(
            lax.dot_general(
                panel[p], flat, (((0,), (0,)), ((), ())), precision=three_pass, preferred_element_type=jnp.float32
            )
        )
    whole = []
    for p in range(pair_dev):
        full = by_layer(
            left[p].reshape(order, width, half_width),
            crossed(left[p], "layer", 1).reshape(order, width, half_width),
            layer_pos,
            2,
        )
        whole.append(full.reshape(order, pair_dev, order))

    line = jnp.stack(downs[:0:-1] + [own] + ups[1:], 0)
    column = jnp.zeros((pair_dev, cols_n, piece, order), jnp.float32)
    for mask in range(cols_n):
        target = col_pos ^ mask
        held = lax.dynamic_index_in_dim(line, row_pos - target + rows_n - 1, 0, keepdims=False)
        if mask:
            held = crossed(held, "col", mask)
        column = lax.dynamic_update_slice(column, held[:, None], (0, col_pos ^ mask, 0, 0))
    split = column.reshape(pair_dev, cols_n, piece, 2, 2, half_width)
    mine = lax.dynamic_index_in_dim(split, layer_pos, 4, keepdims=False)
    theirs = crossed(lax.dynamic_index_in_dim(split, 1 - layer_pos, 4, keepdims=False), "layer", 1)
    right = by_layer(mine, theirs, layer_pos, 2).reshape(pair_dev, order, 2 * half_width)

    rotated = [[None] * width for _ in range(width)]
    moving = [width - 2, 1]
    for slot in moving + [k for k in range(width) if k not in moving]:
        p, m = divmod(slot, 2)
        for q in range(pair_dev):
            lhs = whole[p][m * block_size : (m + 1) * block_size, q]
            out = product(lhs, right[q])
            rotated[slot][2 * q] = out[:, :half_width]
            rotated[slot][2 * q + 1] = out[:, half_width:]

    moved = [None] * width
    for slot in moving + [k for k in range(width) if k not in moving]:
        up = shifted(rotated[slot][width - 2], "col", 1)
        down = shifted(rotated[slot][1], "col", -1)
        moved[slot] = rearranged(rotated[slot], up, down, col_pos, cols_n)
    columns = []
    for j in range(width):
        slots = [moved[k][j] for k in range(width)]
        up = shifted(slots[width - 2], "row", 1)
        down = shifted(slots[1], "row", -1)
        columns.append(jnp.stack(rearranged(slots, up, down, row_pos, rows_n), 0))
    return jnp.stack(columns, 2)


def solution(mesh):
    return jax.shard_map(
        shards,
        mesh=mesh,
        in_specs=(P("row", None, "col", "layer"), P(None, "row", ("col", "layer"), None)),
        out_specs=P("row", None, "col", "layer"),
        check_vma=False,
    )
```

```python
import jax
import jax.numpy as jnp
from jax import lax
from jax.sharding import PartitionSpec as P


three_pass = lax.Precision.HIGH


def shifted(block, axis, distance):
    devices = range(lax.axis_size(axis))
    route = [(i - distance, i) for i in devices if i - distance in devices]
    return lax.ppermute(block, axis, route)


def crossed(block, axis, mask):
    return lax.ppermute(block, axis, [(i, i ^ mask) for i in range(lax.axis_size(axis))])


def rearranged(slots, from_prev, from_next, position, count):
    width = len(slots)
    result = [jnp.where(position == 0, slots[0], from_prev)]
    for local in range(1, width):
        if local % 2 == 1:
            if local == width - 1:
                result.append(jnp.where(position == count - 1, slots[width - 2], from_next))
            else:
                result.append(slots[local + 2])
        else:
            result.append(jnp.where(position == 0, slots[1], slots[0]))
    return result


def by_layer(mine, other, layer_pos, axis):
    low = jnp.where(layer_pos == 0, mine, other)
    high = jnp.where(layer_pos == 0, other, mine)
    return jnp.stack([low, high], axis)


def left_product(panel, flat):
    return lax.dot_general(
        panel, flat, (((0,), (0,)), ((), ())), precision=three_pass, preferred_element_type=jnp.float32
    )


def shards(matrix, transforms):
    width, block_size, _, half_width = matrix.shape
    pair_dev = width // 2
    rows_n = lax.axis_size("row")
    cols_n = lax.axis_size("col")
    row_pos = lax.axis_index("row")
    col_pos = lax.axis_index("col")
    layer_pos = lax.axis_index("layer")
    own = transforms[0]
    piece = own.shape[1]
    order = 2 * block_size

    halves = own.reshape(pair_dev, piece, 2, 2, half_width)
    halves = jnp.stack([halves[:, :, :, h].reshape(pair_dev, piece, block_size) for h in range(2)], 0)

    line = jnp.zeros((2 * rows_n - 1,) + halves.shape, jnp.float32)
    line = lax.dynamic_update_slice(line, halves[None], (rows_n - 1, 0, 0, 0, 0))
    up, down = halves, halves
    hops = []
    for step in range(1, rows_n):
        up = shifted(up, "row", 1)
        down = shifted(down, "row", -1)
        hops.append((step, up, down))

    gathered = jnp.zeros((pair_dev, cols_n, piece, order), jnp.float32)
    for mask in range(cols_n):
        part = own if mask == 0 else crossed(own, "col", mask)
        gathered = lax.dynamic_update_slice(gathered, part[:, None], (0, col_pos ^ mask, 0, 0))
    panel = by_layer(gathered, crossed(gathered, "layer", 1), layer_pos, 2)
    panel = panel.reshape(pair_dev, order, order)

    grouped = matrix.reshape(pair_dev, order, width * half_width)
    left = [left_product(panel[p], grouped[p]).reshape(2, block_size, -1) for p in range(pair_dev)]
    slots = [left[k // 2][k % 2] for k in range(width)]
    moving = [width - 2, 1]
    staying = [k for k in range(width) if k not in moving]
    sets = [jnp.concatenate([slots[k] for k in group], 0) for group in (moving, staying)]
    others = [crossed(part, "layer", 1) for part in sets]

    last_step, last_up, last_down = hops[-1]
    last_up, last_down, *sets = lax.optimization_barrier((last_up, last_down, *sets))
    hops[-1] = (last_step, last_up, last_down)
    for step, up, down in hops:
        line = lax.dynamic_update_slice(line, up[None], (rows_n - 1 + step, 0, 0, 0, 0))
        line = lax.dynamic_update_slice(line, down[None], (rows_n - 1 - step, 0, 0, 0, 0))

    column = jnp.zeros((2, pair_dev, cols_n, piece, block_size), jnp.float32)
    for mask in range(cols_n):
        target = col_pos ^ mask
        held = lax.dynamic_index_in_dim(line, row_pos - target + rows_n - 1, 0, keepdims=False)
        if mask:
            held = crossed(held, "col", mask)
        column = lax.dynamic_update_slice(column, held[:, :, None], (0, 0, col_pos ^ mask, 0, 0))
    mine = lax.dynamic_index_in_dim(column, layer_pos, 0, keepdims=False)
    theirs = crossed(lax.dynamic_index_in_dim(column, 1 - layer_pos, 0, keepdims=False), "layer", 1)
    right = by_layer(mine, theirs, layer_pos, 2).reshape(pair_dev, order, block_size)

    by_half = right.reshape(pair_dev, 2, 2, half_width, block_size)
    right_own, right_other = (
        lax.dynamic_index_in_dim(by_half, at, 2, keepdims=False).reshape(pair_dev, block_size, block_size)
        for at in (layer_pos, 1 - layer_pos)
    )

    def right_product(part, other):
        def one(x, q, r):
            return lax.dot_general(
                x[:, q * block_size : (q + 1) * block_size],
                r[q],
                (((1,), (0,)), ((), ())),
                precision=three_pass,
                preferred_element_type=jnp.float32,
            )

        out = [one(part, q, right_own) + one(other, q, right_other) for q in range(pair_dev)]
        return [out[j // 2][:, (j % 2) * half_width : (j % 2 + 1) * half_width] for j in range(width)]

    def across(cols):
        up = shifted(cols[width - 2], "col", 1)
        down = shifted(cols[1], "col", -1)
        return rearranged(cols, up, down, col_pos, cols_n)

    go = across(right_product(sets[0], others[0]))
    stay = across(right_product(sets[1], others[1]))

    local = [j for j in range(width) if j not in (0, width - 1)]
    columns = [None] * width
    for group in (local, [0, width - 1]):
        both = jnp.stack([go[j] for j in group], 0)
        up = shifted(both[:, :block_size], "row", 1)
        down = shifted(both[:, block_size:], "row", -1)
        for n, j in enumerate(group):
            blocks = [None] * width
            for k, slot in enumerate(moving):
                blocks[slot] = go[j][k * block_size : (k + 1) * block_size]
            for k, slot in enumerate(staying):
                blocks[slot] = stay[j][k * block_size : (k + 1) * block_size]
            columns[j] = jnp.stack(rearranged(blocks, up[n], down[n], row_pos, rows_n), 0)
    return jnp.stack(columns, 2)


def solution(mesh):
    return jax.shard_map(
        shards,
        mesh=mesh,
        in_specs=(P("row", None, "col", "layer"), P(None, "row", ("col", "layer"), None)),
        out_specs=P("row", None, "col", "layer"),
        check_vma=False,
    )
```
